32 devices in a mesh: dp: 8 (over z, core), ctx: 4 (over y, x).
Axes of the slice: x: 2, y: 2, z: 4, core: 2. Of those that a mesh axis runs over, the one named last changes fastest.
Arguments:
- qkv: bfloat16 [8, 512, 5120], P('dp', 'ctx'), may hold values from -8 to 8
- dest: int32 [8, 8], P('dp'), may hold values from 0 to 7, as said below
- order: int32 [8], replicated, may hold values from 0 to 7, as said below
- lengths: int32 [8, 8], replicated, may hold values from 1 to 256, 512 in all within a row
Outputs:
- attended: bfloat16 [8, 512, 4096], P('dp', 'ctx')
The draws below stay inside these ranges and needn't reach their ends.
Inputs may be any that keep to these rules, and one draw needn't show every extreme that they name: `dest`: entry [r, s] is r itself, r + 1 or r - 1 (indices modulo 8), and the relation is mutual: if entry [r, s] is t, entry [t, s] is r. For every c below 4: order[2 c] is below 4 and order[2 c + 1] = 7 - order[2 c]; every span appears once.
All inputs are finite; a program needn't handle non-finite values.
Results may differ from the reference program's by a relative error of at most 0.0031.
Values may be sent and summed in bfloat16 or wider, within the bound.
A program may use at most 64 MiB of HBM per device.

```python
import math
import jax
import jax.numpy as jnp
import numpy as np
from jax import lax

QUERY_HEADS = 32
KEY_VALUE_HEADS = 4
HEAD_SIZE = 128
NDOC = 8
SPAN = 64
QUERIES_PER_KV = 8
WIDTH = 5120
PACKED_LENGTH = 512
MAXDOC = 256
PACKED_COUNT = 8
N_CTX = 4


def draw_dest(key, part):
    parity = jax.random.randint(jax.random.fold_in(key, 11), (2 * N_CTX,), 0, 2)
    flips = jax.random.randint(jax.random.fold_in(key, 12), (PACKED_COUNT, 2 * N_CTX), 0, 2)
    ranks = jnp.arange(PACKED_COUNT, dtype=jnp.int32)[:, None]
    is_lower = (ranks - parity[None, :]) % 2 == 0
    lower_member = jnp.where(is_lower, ranks, ranks - 1) % PACKED_COUNT
    partner = jnp.where(is_lower, ranks + 1, ranks - 1) % PACKED_COUNT
    traded = jnp.take_along_axis(flips, lower_member, axis=0)
    return jnp.where(traded == 1, partner, ranks * jnp.ones_like(partner)).astype(jnp.int32)


def draw_order(key, part):
    early = jax.random.permutation(jax.random.fold_in(key, 21), N_CTX).astype(jnp.int32)
    late = (2 * N_CTX - 1 - early).astype(jnp.int32)
    return jnp.stack([early, late], axis=1).reshape(2 * N_CTX).astype(jnp.int32)


def draw_qkv(key, part):
    random_keys = jax.random.split(jax.random.fold_in(key, 31), 1)
    blank_scores = jax.random.normal(random_keys[0], (PACKED_COUNT, PACKED_LENGTH, WIDTH), jnp.float32)
    return jnp.clip(blank_scores, -8.0, 8.0).astype(jnp.bfloat16)


def profile(number_of, total, most, skew):
    weights = [(1 << 20) // math.isqrt(rank ** skew) + 1 for rank in range(2, number_of + 1)]
    surplus, counts = total - most - (number_of - 1), [1] * (number_of - 1)
    while surplus > 0:
        free = [i for i in range(number_of - 1) if counts[i] < most]
        pool, left = sum([weights[i] for i in free]), surplus
        for i in free:
            addition = min(most - counts[i], max(1, left * weights[i] // pool), surplus)
            counts[i] = counts[i] + addition
            surplus = surplus - addition
    return np.array([most] + counts)


def uneven_parts(own_key, amount, total, limit, lean):
    if amount == 2:
        one = jax.random.randint(own_key, (), max(1, total - limit), min(limit, total - 1) + 1)
        return jnp.stack([one, total - one])
    sizes = jnp.asarray(profile(amount, total, limit, lean), jnp.int32)
    pairs = (amount - 1) // 2
    donor, taker = sizes[1:1 + 2 * pairs:2], sizes[2:2 + 2 * pairs:2]
    slack = jnp.minimum(donor - 1, limit - taker)
    passed = jax.random.randint(jax.random.fold_in(own_key, 1), (pairs,), 0, 1 << 20) % (slack + 1)
    sizes = sizes.at[1:1 + 2 * pairs:2].set(donor - passed).at[2:2 + 2 * pairs:2].set(taker + passed)
    return sizes[jax.random.permutation(jax.random.fold_in(own_key, 2), amount)]


def setup_inputs(seed: int = 0) -> dict:
    streams_of = jax.random.split(jax.random.key(seed), 5)
    qkv = draw_qkv(jax.random.fold_in(streams_of[4], 71), 0)
    dest = draw_dest(jax.random.fold_in(streams_of[4], 71), 0)
    order = draw_order(jax.random.fold_in(streams_of[4], 71), 0)
    lengths = jax.vmap(lambda own: uneven_parts(own, NDOC, PACKED_LENGTH, MAXDOC, 2))(jax.random.split(streams_of[3], PACKED_COUNT)).reshape((PACKED_COUNT, NDOC)).astype(jnp.int32)
    return dict(qkv=qkv, dest=dest, order=order, lengths=lengths)


MASK_FLOOR = -1e+30

def sequence_attention(qkv, dest, order, doc_ends, seq_index):
    row_ids = jnp.arange(PACKED_LENGTH, dtype=jnp.int32)
    row_slot = (row_ids // SPAN).astype(jnp.int32)
    dest_row = lax.dynamic_index_in_dim(dest, seq_index, 0, keepdims=False)
    row_source = jnp.take(dest_row, row_slot).astype(jnp.int32)
    settled = qkv[row_source, row_ids]
    positions = (jnp.take(order, row_slot) * SPAN + row_ids % SPAN).astype(jnp.int32)
    row_ends = jnp.take(doc_ends, row_source, axis=0)
    counted = lax.optimization_barrier(jnp.sum((row_ends <= positions[:, None]).astype(jnp.int32), axis=1))
    documents = (row_source * NDOC + counted).astype(jnp.int32)
    visible = (documents[None, :] == documents[:, None]) & (positions[None, :] <= positions[:, None])
    score_scale = 1.0 / math.sqrt(HEAD_SIZE)
    finished = []
    for head_group_index in range(KEY_VALUE_HEADS):
        query_cols = settled[:, head_group_index * QUERIES_PER_KV * HEAD_SIZE:(head_group_index + 1) * QUERIES_PER_KV * HEAD_SIZE]
        query_block = query_cols.reshape(PACKED_LENGTH, QUERIES_PER_KV, HEAD_SIZE).astype(jnp.float32)
        key_start = QUERY_HEADS * HEAD_SIZE + head_group_index * HEAD_SIZE
        value_offset = (QUERY_HEADS + KEY_VALUE_HEADS) * HEAD_SIZE + head_group_index * HEAD_SIZE
        key_block = settled[:, key_start:key_start + HEAD_SIZE].astype(jnp.float32)
        value_block = settled[:, value_offset:value_offset + HEAD_SIZE].astype(jnp.float32)
        scores = jnp.einsum('qgd,kd->gqk', query_block, key_block, precision=lax.Precision.HIGHEST) * score_scale
        scores = jnp.where(visible[None], scores, MASK_FLOOR)
        row_max = lax.optimization_barrier(jnp.max(scores, axis=2, keepdims=True))
        weights = jnp.where(visible[None], jnp.exp(scores - row_max), 0.0)
        totals = lax.optimization_barrier(jnp.sum(weights, axis=2, keepdims=True))
        rounded = weights.astype(jnp.bfloat16).astype(jnp.float32)
        mixed = jnp.einsum('gqk,kd->gqd', rounded, value_block, precision=lax.Precision.HIGHEST) / totals
        finished.append(jnp.transpose(mixed, (1, 0, 2)).reshape(PACKED_LENGTH, QUERIES_PER_KV * HEAD_SIZE))
    return jnp.concatenate(finished, axis=1).astype(jnp.bfloat16)

def reference(qkv, dest, order, lengths):
    doc_ends = jnp.cumsum(lengths, axis=1).astype(jnp.int32)

    def one_sequence(seq_index):
        return sequence_attention(qkv, dest, order, doc_ends, seq_index)
    return lax.map(one_sequence, jnp.arange(PACKED_COUNT, dtype=jnp.int32))
```

```python
import functools
import math

import jax
import jax.numpy as jnp
from jax import lax
from jax.experimental import pallas as pl
from jax.experimental.pallas import tpu as pltpu
from jax.sharding import PartitionSpec as P

QUERY_HEADS = 32
KEY_VALUE_HEADS = 4
HEAD_SIZE = 128
QUERIES_PER_KV = 8
CHUNK_HEADS = 2

MASK_FLOOR = -1e30
MESH = pl.DeviceIdType.MESH


def kernel(
    dp_count, ctx_count,
    qkv_ref, dest_ref, order_ref, lengths_ref,
    out_ref,
    q_buf, kv_buf, bias, own, from_below, from_above,
    local_sem, kv_send, kv_recv, out_send, out_recv,
):
    dp_index = lax.axis_index("dp")
    me = lax.axis_index("ctx")
    above = lax.rem(dp_index + 1, dp_count)
    below = lax.rem(dp_index + dp_count - 1, dp_count)
    rows = qkv_ref.shape[1]
    span = rows // 2
    docs = lengths_ref.shape[1]
    query_width = QUERY_HEADS * HEAD_SIZE
    chunk_cols = CHUNK_HEADS * HEAD_SIZE
    chunks = QUERY_HEADS // CHUNK_HEADS
    group_chunks = QUERIES_PER_KV // CHUNK_HEADS
    my_rows = pl.ds(pl.multiple_of(me * rows, rows), rows)

    local = []
    for g in range(KEY_VALUE_HEADS):
        for part in range(2):
            first = query_width + (part * KEY_VALUE_HEADS + g) * HEAD_SIZE
            copy = pltpu.make_async_copy(
                qkv_ref.at[0, :, pl.ds(first, HEAD_SIZE)],
                kv_buf.at[g, part, my_rows, :],
                local_sem.at[2 * g + part],
            )
            copy.start()
            local.append(copy)
    q_copy = pltpu.make_async_copy(
        qkv_ref.at[0, :, pl.ds(0, query_width)], q_buf, local_sem.at[2 * KEY_VALUE_HEADS]
    )
    q_copy.start()

    barrier = pltpu.get_barrier_semaphore()
    for k in range(1, ctx_count):
        pl.semaphore_signal(
            barrier, inc=1, device_id={"ctx": lax.rem(me + k, ctx_count)}, device_id_type=MESH
        )
    pl.semaphore_signal(barrier, inc=1, device_id={"dp": above}, device_id_type=MESH)
    pl.semaphore_signal(barrier, inc=1, device_id={"dp": below}, device_id_type=MESH)
    pl.semaphore_wait(barrier, ctx_count + 1)

    def kv_copy(g, k):
        peer = lax.rem(me + k, ctx_count)
        return pltpu.make_async_remote_copy(
            src_ref=kv_buf.at[g, :, my_rows, :],
            dst_ref=kv_buf.at[g, :, my_rows, :],
            send_sem=kv_send.at[g, k],
            recv_sem=kv_recv.at[g, k],
            device_id={"ctx": peer},
            device_id_type=MESH,
        )

    def kv_arrival(g, k):
        peer = lax.rem(me + ctx_count - k, ctx_count)
        its_rows = pl.ds(pl.multiple_of(peer * rows, rows), rows)
        landed = kv_buf.at[g, :, its_rows, :]
        return pltpu.make_async_remote_copy(
            src_ref=landed, dst_ref=landed, send_sem=kv_send.at[g, k], recv_sem=kv_recv.at[g, k],
            device_id={"ctx": peer}, device_id_type=MESH,
        )

    for g in range(KEY_VALUE_HEADS):
        local[2 * g].wait()
        local[2 * g + 1].wait()
        for k in range(1, ctx_count):
            kv_copy(g, k).start()

    ends = []
    total_length = 0
    for d in range(docs):
        total_length = total_length + lengths_ref[dp_index, d]
        ends.append(total_length)

    def identity_of(place, first_slot):
        early = place < span
        position = jnp.where(
            early, order_ref[first_slot] * span, order_ref[first_slot + 1] * span - span
        ) + place
        counted = jnp.where(early, dest_ref[0, first_slot] * docs, dest_ref[0, first_slot + 1] * docs)
        for end in ends:
            counted = counted + (position >= end).astype(jnp.int32)
        return position, counted

    query_place = lax.broadcasted_iota(jnp.int32, (rows, rows), 0)
    key_place = lax.broadcasted_iota(jnp.int32, (rows, rows), 1)
    query_position, query_document = identity_of(query_place, 2 * me)
    for b in range(ctx_count):
        key_position, key_document = identity_of(key_place, 2 * b)
        visible = (key_document == query_document) & (key_position <= query_position)
        bias[:, b * rows:(b + 1) * rows] = jnp.where(visible, 0.0, MASK_FLOOR)

    def out_copy(chunk, up):
        return pltpu.make_async_remote_copy(
            src_ref=own.at[chunk],
            dst_ref=(from_below if up else from_above).at[chunk],
            send_sem=out_send.at[up, chunk],
            recv_sem=out_recv.at[up, chunk],
            device_id={"dp": above if up else below},
            device_id_type=MESH,
        )

    def send(chunk):
        out_copy(chunk, 1).start()
        out_copy(chunk, 0).start()

    exponent_scale = math.log2(math.e) / math.sqrt(HEAD_SIZE)
    q_copy.wait()
    for g in range(KEY_VALUE_HEADS):
        for k in range(1, ctx_count):
            kv_arrival(g, k).wait_recv()

        def one_chunk(i, carry):
            chunk = g * group_chunks + i
            for j in range(CHUNK_HEADS):
                first = pl.multiple_of(chunk * chunk_cols + j * HEAD_SIZE, HEAD_SIZE)
                query = q_buf[:, pl.ds(first, HEAD_SIZE)]
                scores = lax.dot_general(
                    query, kv_buf[g, 0], (((1,), (1,)), ((), ())),
                    preferred_element_type=jnp.float32,
                ) + bias[...]
                row_max = jnp.max(scores, axis=1, keepdims=True)
                weights = jnp.exp2((scores - row_max) * exponent_scale)
                total = jnp.sum(weights, axis=1, keepdims=True)
                mixed = jnp.dot(
                    weights.astype(jnp.bfloat16), kv_buf[g, 1],
                    preferred_element_type=jnp.float32,
                )
                own[chunk, :, j * HEAD_SIZE:(j + 1) * HEAD_SIZE] = (mixed / total).astype(jnp.bfloat16)
                if j == 0:
                    if g == 0:
                        @pl.when(i > 0)
                        def _():
                            send(chunk - 1)
                    else:
                        send(chunk - 1)
            return carry

        lax.fori_loop(0, group_chunks, one_chunk, 0)
    send(chunks - 1)

    below_masks, above_masks = [], []
    for half in range(2):
        source = jnp.full((span, chunk_cols), dest_ref[0, 2 * me + half], jnp.int32)
        below_masks.append(source == below)
        above_masks.append(source == above)

    def settle(chunk, carry):
        out_copy(chunk, 1).wait_recv()
        out_copy(chunk, 0).wait_recv()
        first = pl.multiple_of(chunk * chunk_cols, chunk_cols)
        for half in range(2):
            part = pl.ds(half * span, span)
            kept = own[chunk, part, :].astype(jnp.float32)
            lower = from_below[chunk, part, :].astype(jnp.float32)
            upper = from_above[chunk, part, :].astype(jnp.float32)
            chosen = jnp.where(
                below_masks[half], lower, jnp.where(above_masks[half], upper, kept)
            )
            out_ref[0, part, pl.ds(first, chunk_cols)] = chosen.astype(jnp.bfloat16)
        return carry

    lax.fori_loop(0, chunks, settle, 0)

    for g in range(KEY_VALUE_HEADS):
        for k in range(1, ctx_count):
            kv_copy(g, k).wait_send()

    def drain(chunk, carry):
        out_copy(chunk, 1).wait_send()
        out_copy(chunk, 0).wait_send()
        return carry

    lax.fori_loop(0, chunks, drain, 0)


def on_device(dp_count, ctx_count, qkv, dest, order, lengths):
    rows = qkv.shape[1]
    query_width = QUERY_HEADS * HEAD_SIZE
    chunks = QUERY_HEADS // CHUNK_HEADS
    chunk_shape = (chunks, rows, CHUNK_HEADS * HEAD_SIZE)
    keys = ctx_count * rows
    return pl.pallas_call(
        functools.partial(kernel, dp_count, ctx_count),
        out_shape=jax.ShapeDtypeStruct((1, rows, query_width), jnp.bfloat16),
        in_specs=[
            pl.BlockSpec(memory_space=pl.ANY),
            pl.BlockSpec(memory_space=pltpu.SMEM),
            pl.BlockSpec(memory_space=pltpu.SMEM),
            pl.BlockSpec(memory_space=pltpu.SMEM),
        ],
        out_specs=pl.BlockSpec(memory_space=pltpu.VMEM),
        scratch_shapes=[
            pltpu.VMEM((rows, query_width), jnp.bfloat16),
            pltpu.VMEM((KEY_VALUE_HEADS, 2, keys, HEAD_SIZE), jnp.bfloat16),
            pltpu.VMEM((rows, keys), jnp.float32),
            pltpu.VMEM(chunk_shape, jnp.bfloat16),
            pltpu.VMEM(chunk_shape, jnp.bfloat16),
            pltpu.VMEM(chunk_shape, jnp.bfloat16),
            pltpu.SemaphoreType.DMA((2 * KEY_VALUE_HEADS + 1,)),
            pltpu.SemaphoreType.DMA((KEY_VALUE_HEADS, ctx_count)),
            pltpu.SemaphoreType.DMA((KEY_VALUE_HEADS, ctx_count)),
            pltpu.SemaphoreType.DMA((2, chunks)),
            pltpu.SemaphoreType.DMA((2, chunks)),
        ],
        compiler_params=pltpu.CompilerParams(collective_id=0, has_side_effects=True),
    )(qkv, dest, order, lengths)


def solution(mesh):
    return jax.shard_map(
        functools.partial(on_device, mesh.shape["dp"], mesh.shape["ctx"]),
        mesh=mesh,
        in_specs=(P("dp", "ctx", None), P("dp", None), P(), P()),
        out_specs=P("dp", "ctx", None),
        check_vma=False,
    )
```

```python
import functools
import math

import jax
import jax.numpy as jnp
from jax import lax
from jax.experimental import pallas as pl
from jax.experimental.pallas import tpu as pltpu
from jax.sharding import PartitionSpec as P

QUERY_HEADS = 32
KEY_VALUE_HEADS = 4
HEAD_SIZE = 128
QUERIES_PER_KV = 8
CHUNK_HEADS = 2
PLACE_PARTS = 4

MASK_FLOOR = -1e30
MESH = pl.DeviceIdType.MESH


def kernel(
    dp_count, ctx_count,
    qkv_ref, dest_hbm, order_hbm, lengths_hbm,
    out_ref,
    dest_ref, order_ref, lengths_ref, q_buf, kv_buf, bias, own, from_below, from_above,
    local_sem, scalar_sem, kv_send, kv_recv, out_send, out_recv,
):
    dp_index = lax.axis_index("dp")
    me = lax.axis_index("ctx")
    above = lax.rem(dp_index + 1, dp_count)
    below = lax.rem(dp_index + dp_count - 1, dp_count)
    rows = qkv_ref.shape[1]
    span = rows // 2
    docs = lengths_ref.shape[1]
    query_width = QUERY_HEADS * HEAD_SIZE
    chunk_cols = CHUNK_HEADS * HEAD_SIZE
    chunks = QUERY_HEADS // CHUNK_HEADS
    group_chunks = QUERIES_PER_KV // CHUNK_HEADS
    my_rows = pl.ds(pl.multiple_of(me * rows, rows), rows)

    barrier = pltpu.get_barrier_semaphore()
    for k in range(1, ctx_count):
        pl.semaphore_signal(
            barrier, inc=1, device_id={"ctx": lax.rem(me + k, ctx_count)}, device_id_type=MESH
        )
    pl.semaphore_signal(barrier, inc=1, device_id={"dp": above}, device_id_type=MESH)
    pl.semaphore_signal(barrier, inc=1, device_id={"dp": below}, device_id_type=MESH)
    scalars = [
        pltpu.make_async_copy(source, target, scalar_sem.at[i])
        for i, (source, target) in enumerate(
            ((dest_hbm, dest_ref), (order_hbm, order_ref), (lengths_hbm, lengths_ref))
        )
    ]
    local = []
    for g in range(KEY_VALUE_HEADS):
        for part in range(2):
            first = query_width + (part * KEY_VALUE_HEADS + g) * HEAD_SIZE
            copy = pltpu.make_async_copy(
                qkv_ref.at[0, :, pl.ds(first, HEAD_SIZE)],
                kv_buf.at[g, part, my_rows, :],
                local_sem.at[2 * g + part],
            )
            copy.start()
            local.append(copy)
    q_copy = pltpu.make_async_copy(
        qkv_ref.at[0, :, pl.ds(0, query_width)], q_buf, local_sem.at[2 * KEY_VALUE_HEADS]
    )
    q_copy.start()
    for copy in scalars:
        copy.start()

    pl.semaphore_wait(barrier, ctx_count + 1)

    def kv_copy(g, k):
        peer = lax.rem(me + k, ctx_count)
        return pltpu.make_async_remote_copy(
            src_ref=kv_buf.at[g, :, my_rows, :],
            dst_ref=kv_buf.at[g, :, my_rows, :],
            send_sem=kv_send.at[g, k],
            recv_sem=kv_recv.at[g, k],
            device_id={"ctx": peer},
            device_id_type=MESH,
        )

    def kv_arrival(g, k):
        peer = lax.rem(me + ctx_count - k, ctx_count)
        its_rows = pl.ds(pl.multiple_of(peer * rows, rows), rows)
        landed = kv_buf.at[g, :, its_rows, :]
        return pltpu.make_async_remote_copy(
            src_ref=landed, dst_ref=landed, send_sem=kv_send.at[g, k], recv_sem=kv_recv.at[g, k],
            device_id={"ctx": peer}, device_id_type=MESH,
        )

    for g in range(KEY_VALUE_HEADS):
        local[2 * g].wait()
        local[2 * g + 1].wait()
        for k in range(1, ctx_count):
            kv_copy(g, k).start()

    for copy in scalars:
        copy.wait()

    ends = []
    total_length = 0
    for d in range(docs):
        total_length = total_length + lengths_ref[dp_index, d]
        ends.append(total_length)

    def identity_of(place, first_slot):
        early = place < span
        position = jnp.where(
            early, order_ref[first_slot] * span, order_ref[first_slot + 1] * span - span
        ) + place
        counted = jnp.where(early, dest_ref[0, first_slot] * docs, dest_ref[0, first_slot + 1] * docs)
        for end in ends:
            counted = counted + (position >= end).astype(jnp.int32)
        return position, counted

    query_place = lax.broadcasted_iota(jnp.int32, (rows, rows), 0)
    key_place = lax.broadcasted_iota(jnp.int32, (rows, rows), 1)
    query_position, query_document = identity_of(query_place, 2 * me)
    for b in range(ctx_count):
        key_position, key_document = identity_of(key_place, 2 * b)
        visible = (key_document == query_document) & (key_position <= query_position)
        bias[:, b * rows:(b + 1) * rows] = jnp.where(visible, 0.0, MASK_FLOOR)

    def out_copy(chunk, up):
        return pltpu.make_async_remote_copy(
            src_ref=own.at[chunk],
            dst_ref=(from_below if up else from_above).at[chunk],
            send_sem=out_send.at[up, chunk],
            recv_sem=out_recv.at[up, chunk],
            device_id={"dp": above if up else below},
            device_id_type=MESH,
        )

    def send(chunk):
        out_copy(chunk, 1).start()
        out_copy(chunk, 0).start()

    exponent_scale = math.log2(math.e) / math.sqrt(HEAD_SIZE)
    q_copy.wait()
    for g in range(KEY_VALUE_HEADS):
        for k in range(1, ctx_count):
            kv_arrival(g, k).wait_recv()

        def one_chunk(i, carry):
            chunk = g * group_chunks + i
            for j in range(CHUNK_HEADS):
                first = pl.multiple_of(chunk * chunk_cols + j * HEAD_SIZE, HEAD_SIZE)
                query = q_buf[:, pl.ds(first, HEAD_SIZE)]
                scores = lax.dot_general(
                    query, kv_buf[g, 0], (((1,), (1,)), ((), ())),
                    preferred_element_type=jnp.float32,
                ) + bias[...]
                row_max = jnp.max(scores, axis=1, keepdims=True)
                weights = jnp.exp2((scores - row_max) * exponent_scale)
                total = jnp.sum(weights, axis=1, keepdims=True)
                mixed = jnp.dot(
                    weights.astype(jnp.bfloat16), kv_buf[g, 1],
                    preferred_element_type=jnp.float32,
                )
                own[chunk, :, j * HEAD_SIZE:(j + 1) * HEAD_SIZE] = (mixed / total).astype(jnp.bfloat16)
                if j == 0:
                    if g == 0:
                        @pl.when(i > 0)
                        def _():
                            send(chunk - 1)
                    else:
                        send(chunk - 1)
            return carry

        lax.fori_loop(0, group_chunks, one_chunk, 0)
    send(chunks - 1)

    below_masks, above_masks = [], []
    for half in range(2):
        source = jnp.full((span, chunk_cols), dest_ref[0, 2 * me + half], jnp.int32)
        below_masks.append(source == below)
        above_masks.append(source == above)

    def settle(chunk, carry):
        out_copy(chunk, 1).wait_recv()
        out_copy(chunk, 0).wait_recv()
        first = pl.multiple_of(chunk * chunk_cols, chunk_cols)
        for half in range(2):
            part = pl.ds(half * span, span)
            kept = own[chunk, part, :].astype(jnp.float32)
            lower = from_below[chunk, part, :].astype(jnp.float32)
            upper = from_above[chunk, part, :].astype(jnp.float32)
            chosen = jnp.where(
                below_masks[half], lower, jnp.where(above_masks[half], upper, kept)
            )
            out_ref[0, part, pl.ds(first, chunk_cols)] = chosen.astype(jnp.bfloat16)
        return carry

    lax.fori_loop(0, chunks, settle, 0)

    for g in range(KEY_VALUE_HEADS):
        for k in range(1, ctx_count):
            kv_copy(g, k).wait_send()

    def drain(chunk, carry):
        out_copy(chunk, 1).wait_send()
        out_copy(chunk, 0).wait_send()
        return carry

    lax.fori_loop(0, chunks, drain, 0)


def place_kernel(settled_ref, out_ref, sems):
    rows = settled_ref.shape[1] // PLACE_PARTS
    copies = [
        pltpu.make_async_copy(
            settled_ref.at[0, pl.ds(i * rows, rows), :],
            out_ref.at[0, pl.ds(i * rows, rows), :],
            sems.at[i],
        )
        for i in range(PLACE_PARTS)
    ]
    for copy in copies:
        copy.start()
    for copy in copies:
        copy.wait()


def on_device(dp_count, ctx_count, qkv, dest, order, lengths):
    rows = qkv.shape[1]
    query_width = QUERY_HEADS * HEAD_SIZE
    chunks = QUERY_HEADS // CHUNK_HEADS
    chunk_shape = (chunks, rows, CHUNK_HEADS * HEAD_SIZE)
    keys = ctx_count * rows
    qkv, dest, order, lengths = (
        pltpu.with_memory_space_constraint(array, pltpu.HBM)
        for array in (qkv, dest, order, lengths)
    )
    settled = pl.pallas_call(
        functools.partial(kernel, dp_count, ctx_count),
        out_shape=pltpu.VMEM((1, rows, query_width), jnp.bfloat16),
        in_specs=[pl.BlockSpec(memory_space=pltpu.HBM)] * 4,
        out_specs=pl.BlockSpec(memory_space=pltpu.VMEM),
        scratch_shapes=[
            pltpu.SMEM(dest.shape, jnp.int32),
            pltpu.SMEM(order.shape, jnp.int32),
            pltpu.SMEM(lengths.shape, jnp.int32),
            pltpu.VMEM((rows, query_width), jnp.bfloat16),
            pltpu.VMEM((KEY_VALUE_HEADS, 2, keys, HEAD_SIZE), jnp.bfloat16),
            pltpu.VMEM((rows, keys), jnp.float32),
            pltpu.VMEM(chunk_shape, jnp.bfloat16),
            pltpu.VMEM(chunk_shape, jnp.bfloat16),
            pltpu.VMEM(chunk_shape, jnp.bfloat16),
            pltpu.SemaphoreType.DMA((2 * KEY_VALUE_HEADS + 1,)),
            pltpu.SemaphoreType.DMA((3,)),
            pltpu.SemaphoreType.DMA((KEY_VALUE_HEADS, ctx_count)),
            pltpu.SemaphoreType.DMA((KEY_VALUE_HEADS, ctx_count)),
            pltpu.SemaphoreType.DMA((2, chunks)),
            pltpu.SemaphoreType.DMA((2, chunks)),
        ],
        compiler_params=pltpu.CompilerParams(collective_id=0, has_side_effects=True,
            vmem_limit_bytes=40 << 20),
    )(qkv, dest, order, lengths)
    return pl.pallas_call(
        place_kernel,
        out_shape=jax.ShapeDtypeStruct((1, rows, query_width), jnp.bfloat16),
        in_specs=[pl.BlockSpec(memory_space=pltpu.VMEM)],
        out_specs=pl.BlockSpec(memory_space=pltpu.HBM),
        scratch_shapes=[pltpu.SemaphoreType.DMA((PLACE_PARTS,))],
        compiler_params=pltpu.CompilerParams(vmem_limit_bytes=8 << 20),
    )(settled)


def solution(mesh):
    return jax.shard_map(
        functools.partial(on_device, mesh.shape["dp"], mesh.shape["ctx"]),
        mesh=mesh,
        in_specs=(P("dp", "ctx", None), P("dp", None), P(), P()),
        out_specs=P("dp", "ctx", None),
        check_vma=False,
    )
```

```python
import functools
import math

import jax
import jax.numpy as jnp
from jax import lax
from jax.experimental import pallas as pl
from jax.experimental.pallas import tpu as pltpu
from jax.sharding import PartitionSpec as P

QUERY_HEADS = 32
KEY_VALUE_HEADS = 4
HEAD_SIZE = 128
QUERIES_PER_KV = 8
CHUNK_HEADS = 2
PLACE_PARTS = 4

MASK_FLOOR = -1e30
MESH = pl.DeviceIdType.MESH


def kernel(
    dp_count, ctx_count,
    qkv_ref, dest_hbm, order_hbm, lengths_hbm,
    out_ref,
    dest_ref, order_ref, lengths_ref, q_buf, kv_buf, bias, settled_bias, own, from_below, from_above,
    moved_q, moved_kv, own_kv,
    local_sem, scalar_sem, kv_send, kv_recv, out_send, out_recv, moved_send, moved_recv,
):
    dp_index = lax.axis_index("dp")
    me = lax.axis_index("ctx")
    above = lax.rem(dp_index + 1, dp_count)
    below = lax.rem(dp_index + dp_count - 1, dp_count)
    rows = qkv_ref.shape[1]
    span = rows // 2
    docs = lengths_ref.shape[1]
    query_width = QUERY_HEADS * HEAD_SIZE
    chunk_cols = CHUNK_HEADS * HEAD_SIZE
    moved = KEY_VALUE_HEADS - 1
    group_chunks = QUERIES_PER_KV // CHUNK_HEADS
    chunks = moved * group_chunks
    moved_cols = pl.ds(moved * QUERIES_PER_KV * HEAD_SIZE, QUERIES_PER_KV * HEAD_SIZE)
    my_rows = pl.ds(pl.multiple_of(me * rows, rows), rows)

    barrier = pltpu.get_barrier_semaphore()
    for k in range(1, ctx_count):
        pl.semaphore_signal(
            barrier, inc=1, device_id={"ctx": lax.rem(me + k, ctx_count)}, device_id_type=MESH
        )
    pl.semaphore_signal(barrier, inc=1, device_id={"dp": above}, device_id_type=MESH)
    pl.semaphore_signal(barrier, inc=1, device_id={"dp": below}, device_id_type=MESH)
    scalars = [
        pltpu.make_async_copy(source, target, scalar_sem.at[i])
        for i, (source, target) in enumerate(
            ((dest_hbm, dest_ref), (order_hbm, order_ref), (lengths_hbm, lengths_ref))
        )
    ]
    local = []
    for g in (moved, *range(moved)):
        for part in range(2):
            first = query_width + (part * KEY_VALUE_HEADS + g) * HEAD_SIZE
            copy = pltpu.make_async_copy(
                qkv_ref.at[0, :, pl.ds(first, HEAD_SIZE)],
                own_kv.at[part] if g == moved else kv_buf.at[g, part, my_rows, :],
                local_sem.at[2 * g + part],
            )
            copy.start()
            local.append(copy)
        if g == moved:
            q_copy = pltpu.make_async_copy(
                qkv_ref.at[0, :, pl.ds(0, query_width)], q_buf, local_sem.at[2 * KEY_VALUE_HEADS]
            )
            q_copy.start()
    for copy in scalars:
        copy.start()

    pl.semaphore_wait(barrier, ctx_count + 1)

    def kv_copy(g, k):
        peer = lax.rem(me + k, ctx_count)
        return pltpu.make_async_remote_copy(
            src_ref=kv_buf.at[g, :, my_rows, :],
            dst_ref=kv_buf.at[g, :, my_rows, :],
            send_sem=kv_send.at[g, k],
            recv_sem=kv_recv.at[g, k],
            device_id={"ctx": peer},
            device_id_type=MESH,
        )

    def kv_arrival(g, k):
        peer = lax.rem(me + ctx_count - k, ctx_count)
        its_rows = pl.ds(pl.multiple_of(peer * rows, rows), rows)
        landed = kv_buf.at[g, :, its_rows, :]
        return pltpu.make_async_remote_copy(
            src_ref=landed, dst_ref=landed, send_sem=kv_send.at[g, k], recv_sem=kv_recv.at[g, k],
            device_id={"ctx": peer}, device_id_type=MESH,
        )

    def moved_copy(kind, up):
        return pltpu.make_async_remote_copy(
            src_ref=q_buf.at[:, moved_cols] if kind else own_kv,
            dst_ref=(moved_q if kind else moved_kv).at[up],
            send_sem=moved_send.at[up, kind],
            recv_sem=moved_recv.at[up, kind],
            device_id={"dp": above if up else below},
            device_id_type=MESH,
        )

    local[0].wait()
    local[1].wait()
    moved_copy(0, 1).start()
    moved_copy(0, 0).start()
    for g in range(moved):
        local[2 * g + 2].wait()
        local[2 * g + 3].wait()
        for k in range(1, ctx_count):
            kv_copy(g, k).start()
        if g == 0:
            q_copy.wait()
            moved_copy(1, 1).start()
            moved_copy(1, 0).start()

    for copy in scalars:
        copy.wait()

    def ends_of(sequence):
        ends = []
        total_length = 0
        for d in range(docs):
            total_length = total_length + lengths_ref[sequence, d]
            ends.append(total_length)
        return ends

    own_ends = ends_of(dp_index)

    def identity_of(place, first_slot, settled):
        early = place < span
        position = jnp.where(
            early, order_ref[first_slot] * span, order_ref[first_slot + 1] * span - span
        ) + place
        partners = dest_ref[0, first_slot], dest_ref[0, first_slot + 1]
        counted = jnp.where(early, partners[0] * docs, partners[1] * docs)
        if settled:
            ends = [jnp.where(early, *pair) for pair in zip(ends_of(partners[0]), ends_of(partners[1]))]
        else:
            ends = own_ends
        for end in ends:
            counted = counted + (position >= end).astype(jnp.int32)
        return position, counted

    query_place = lax.broadcasted_iota(jnp.int32, (rows, rows), 0)
    key_place = lax.broadcasted_iota(jnp.int32, (1, rows), 1)
    for settled, target in ((False, bias), (True, settled_bias)):
        query_position, query_document = identity_of(query_place, 2 * me, settled)
        for b in range(ctx_count):
            key_position, key_document = identity_of(key_place, 2 * b, settled)
            visible = (key_document == query_document) & (key_position <= query_position)
            target[:, b * rows:(b + 1) * rows] = jnp.where(visible, 0.0, MASK_FLOOR)

    row_source = jnp.where(
        lax.broadcasted_iota(jnp.int32, (rows, HEAD_SIZE), 0) < span,
        dest_ref[0, 2 * me], dest_ref[0, 2 * me + 1],
    )
    is_below = row_source == below
    is_above = row_source == above

    def settle_rows(kept, lower, upper):
        chosen = jnp.where(
            is_below, lower.astype(jnp.float32),
            jnp.where(is_above, upper.astype(jnp.float32), kept.astype(jnp.float32)),
        )
        return chosen.astype(jnp.bfloat16)

    def out_copy(chunk, up):
        return pltpu.make_async_remote_copy(
            src_ref=own.at[chunk],
            dst_ref=(from_below if up else from_above).at[chunk],
            send_sem=out_send.at[up, chunk],
            recv_sem=out_recv.at[up, chunk],
            device_id={"dp": above if up else below},
            device_id_type=MESH,
        )

    def send(chunk):
        out_copy(chunk, 1).start()
        out_copy(chunk, 0).start()

    exponent_scale = math.log2(math.e) / math.sqrt(HEAD_SIZE)

    def attend(query, g, mask):
        scores = lax.dot_general(
            query, kv_buf[g, 0], (((1,), (1,)), ((), ())), preferred_element_type=jnp.float32
        ) + mask[...]
        row_max = jnp.max(scores, axis=1, keepdims=True)
        weights = jnp.exp2((scores - row_max) * exponent_scale)
        total = jnp.sum(weights, axis=1, keepdims=True)
        mixed = jnp.dot(
            weights.astype(jnp.bfloat16), kv_buf[g, 1], preferred_element_type=jnp.float32
        )
        return (mixed / total).astype(jnp.bfloat16)

    for g in range(moved):
        for k in range(1, ctx_count):
            kv_arrival(g, k).wait_recv()

        def one_chunk(i, carry):
            chunk = g * group_chunks + i
            for j in range(CHUNK_HEADS):
                first = pl.multiple_of(chunk * chunk_cols + j * HEAD_SIZE, HEAD_SIZE)
                own[chunk, :, j * HEAD_SIZE:(j + 1) * HEAD_SIZE] = attend(
                    q_buf[:, pl.ds(first, HEAD_SIZE)], g, bias
                )
                if j == 0:
                    if g == 0:
                        @pl.when(i > 0)
                        def _():
                            send(chunk - 1)
                    else:
                        send(chunk - 1)
            return carry

        if g == moved - 1:
            for k in range(1, ctx_count):
                kv_copy(moved, k).start()
        lax.fori_loop(0, group_chunks, one_chunk, 0)
        if g == max(moved - 2, 0):
            moved_copy(0, 1).wait_recv()
            moved_copy(0, 0).wait_recv()
            for part in range(2):
                kv_buf[moved, part, my_rows, :] = settle_rows(
                    own_kv[part], moved_kv[1, part], moved_kv[0, part]
                )
    send(chunks - 1)

    moved_copy(1, 1).wait_recv()
    moved_copy(1, 0).wait_recv()
    for k in range(1, ctx_count):
        kv_arrival(moved, k).wait_recv()

    def one_moved(i, carry):
        for j in range(CHUNK_HEADS):
            inner = pl.ds(pl.multiple_of(i * chunk_cols + j * HEAD_SIZE, HEAD_SIZE), HEAD_SIZE)
            outer = pl.ds(
                pl.multiple_of(chunks * chunk_cols + i * chunk_cols + j * HEAD_SIZE, HEAD_SIZE),
                HEAD_SIZE,
            )
            query = settle_rows(q_buf[:, outer], moved_q[1, :, inner], moved_q[0, :, inner])
            out_ref[0, :, outer] = attend(query, moved, settled_bias)
        return carry

    lax.fori_loop(0, group_chunks, one_moved, 0)

    def settle(chunk, carry):
        out_copy(chunk, 1).wait_recv()
        out_copy(chunk, 0).wait_recv()
        for j in range(CHUNK_HEADS):
            first = pl.multiple_of(chunk * chunk_cols + j * HEAD_SIZE, HEAD_SIZE)
            part = pl.ds(j * HEAD_SIZE, HEAD_SIZE)
            out_ref[0, :, pl.ds(first, HEAD_SIZE)] = settle_rows(
                own[chunk, :, part], from_below[chunk, :, part], from_above[chunk, :, part]
            )
        return carry

    lax.fori_loop(0, chunks, settle, 0)

    for kind in range(2):
        for up in range(2):
            moved_copy(kind, up).wait_send()
    for g in range(KEY_VALUE_HEADS):
        for k in range(1, ctx_count):
            kv_copy(g, k).wait_send()

    def drain(chunk, carry):
        out_copy(chunk, 1).wait_send()
        out_copy(chunk, 0).wait_send()
        return carry

    lax.fori_loop(0, chunks, drain, 0)


def place_kernel(settled_ref, out_ref, sems):
    rows = settled_ref.shape[1] // PLACE_PARTS
    copies = [
        pltpu.make_async_copy(
            settled_ref.at[0, pl.ds(i * rows, rows), :],
            out_ref.at[0, pl.ds(i * rows, rows), :],
            sems.at[i],
        )
        for i in range(PLACE_PARTS)
    ]
    for copy in copies:
        copy.start()
    for copy in copies:
        copy.wait()


def on_device(dp_count, ctx_count, qkv, dest, order, lengths):
    rows = qkv.shape[1]
    query_width = QUERY_HEADS * HEAD_SIZE
    group_width = QUERIES_PER_KV * HEAD_SIZE
    chunks = (QUERY_HEADS - QUERIES_PER_KV) // CHUNK_HEADS
    chunk_shape = (chunks, rows, CHUNK_HEADS * HEAD_SIZE)
    keys = ctx_count * rows
    qkv, dest, order, lengths = (
        pltpu.with_memory_space_constraint(array, pltpu.HBM)
        for array in (qkv, dest, order, lengths)
    )
    settled = pl.pallas_call(
        functools.partial(kernel, dp_count, ctx_count),
        out_shape=pltpu.VMEM((1, rows, query_width), jnp.bfloat16),
        in_specs=[pl.BlockSpec(memory_space=pltpu.HBM)] * 4,
        out_specs=pl.BlockSpec(memory_space=pltpu.VMEM),
        scratch_shapes=[
            pltpu.SMEM(dest.shape, jnp.int32),
            pltpu.SMEM(order.shape, jnp.int32),
            pltpu.SMEM(lengths.shape, jnp.int32),
            pltpu.VMEM((rows, query_width), jnp.bfloat16),
            pltpu.VMEM((KEY_VALUE_HEADS, 2, keys, HEAD_SIZE), jnp.bfloat16),
            pltpu.VMEM((rows, keys), jnp.float32),
            pltpu.VMEM((rows, keys), jnp.float32),
            pltpu.VMEM(chunk_shape, jnp.bfloat16),
            pltpu.VMEM(chunk_shape, jnp.bfloat16),
            pltpu.VMEM(chunk_shape, jnp.bfloat16),
            pltpu.VMEM((2, rows, group_width), jnp.bfloat16),
            pltpu.VMEM((2, 2, rows, HEAD_SIZE), jnp.bfloat16),
            pltpu.VMEM((2, rows, HEAD_SIZE), jnp.bfloat16),
            pltpu.SemaphoreType.DMA((2 * KEY_VALUE_HEADS + 1,)),
            pltpu.SemaphoreType.DMA((3,)),
            pltpu.SemaphoreType.DMA((KEY_VALUE_HEADS, ctx_count)),
            pltpu.SemaphoreType.DMA((KEY_VALUE_HEADS, ctx_count)),
            pltpu.SemaphoreType.DMA((2, chunks)),
            pltpu.SemaphoreType.DMA((2, chunks)),
            pltpu.SemaphoreType.DMA((2, 2)),
            pltpu.SemaphoreType.DMA((2, 2)),
        ],
        compiler_params=pltpu.CompilerParams(collective_id=0, has_side_effects=True,
            vmem_limit_bytes=40 << 20),
    )(qkv, dest, order, lengths)
    return pl.pallas_call(
        place_kernel,
        out_shape=jax.ShapeDtypeStruct((1, rows, query_width), jnp.bfloat16),
        in_specs=[pl.BlockSpec(memory_space=pltpu.VMEM)],
        out_specs=pl.BlockSpec(memory_space=pltpu.HBM),
        scratch_shapes=[pltpu.SemaphoreType.DMA((PLACE_PARTS,))],
        compiler_params=pltpu.CompilerParams(vmem_limit_bytes=8 << 20),
    )(settled)


def solution(mesh):
    return jax.shard_map(
        functools.partial(on_device, mesh.shape["dp"], mesh.shape["ctx"]),
        mesh=mesh,
        in_specs=(P("dp", "ctx", None), P("dp", None), P(), P()),
        out_specs=P("dp", "ctx", None),
        check_vma=False,
    )
```

```python
import functools
import math

import jax
import jax.numpy as jnp
from jax import lax
from jax.experimental import pallas as pl
from jax.experimental.pallas import tpu as pltpu
from jax.sharding import PartitionSpec as P

QUERY_HEADS = 32
KEY_VALUE_HEADS = 4
HEAD_SIZE = 128
QUERIES_PER_KV = 8
CHUNK_HEADS = 4
PLACE_PARTS = 4

MASK_FLOOR = -1e30
MESH = pl.DeviceIdType.MESH


def kernel(
    dp_count, ctx_count,
    qkv_ref, dest_hbm, order_hbm, lengths_hbm,
    out_ref,
    dest_ref, order_ref, lengths_ref, q_buf, kv_buf, bias, settled_bias, own, from_below, from_above,
    moved_q, moved_kv, own_kv,
    local_sem, scalar_sem, kv_send, kv_recv, out_send, out_recv, moved_send, moved_recv,
):
    dp_index = lax.axis_index("dp")
    me = lax.axis_index("ctx")
    above = lax.rem(dp_index + 1, dp_count)
    below = lax.rem(dp_index + dp_count - 1, dp_count)
    rows = qkv_ref.shape[1]
    span = rows // 2
    docs = lengths_ref.shape[1]
    query_width = QUERY_HEADS * HEAD_SIZE
    chunk_cols = CHUNK_HEADS * HEAD_SIZE
    moved = KEY_VALUE_HEADS - 1
    group_chunks = QUERIES_PER_KV // CHUNK_HEADS
    chunks = moved * group_chunks
    moved_cols = pl.ds(moved * QUERIES_PER_KV * HEAD_SIZE, QUERIES_PER_KV * HEAD_SIZE)
    my_rows = pl.ds(pl.multiple_of(me * rows, rows), rows)

    barrier = pltpu.get_barrier_semaphore()
    pl.semaphore_signal(barrier, inc=1, device_id={"dp": above}, device_id_type=MESH)
    pl.semaphore_signal(barrier, inc=1, device_id={"dp": below}, device_id_type=MESH)
    for k in range(1, ctx_count):
        pl.semaphore_signal(
            barrier, inc=1, device_id={"ctx": lax.rem(me + k, ctx_count)}, device_id_type=MESH
        )
    scalars = [
        pltpu.make_async_copy(source, target, scalar_sem.at[i])
        for i, (source, target) in enumerate(
            ((dest_hbm, dest_ref), (order_hbm, order_ref), (lengths_hbm, lengths_ref))
        )
    ]
    local = []
    for g in (moved, *range(moved)):
        for part in range(2):
            first = query_width + (part * KEY_VALUE_HEADS + g) * HEAD_SIZE
            copy = pltpu.make_async_copy(
                qkv_ref.at[0, :, pl.ds(first, HEAD_SIZE)],
                own_kv.at[part] if g == moved else kv_buf.at[g, part, my_rows, :],
                local_sem.at[2 * g + part],
            )
            copy.start()
            local.append(copy)
        if g == moved:
            q_copy = pltpu.make_async_copy(
                qkv_ref.at[0, :, pl.ds(0, query_width)], q_buf, local_sem.at[2 * KEY_VALUE_HEADS]
            )
            q_copy.start()
    for copy in scalars:
        copy.start()

    pl.semaphore_wait(barrier, ctx_count + 1)

    def kv_copy(g, k):
        peer = lax.rem(me + k, ctx_count)
        return pltpu.make_async_remote_copy(
            src_ref=kv_buf.at[g, :, my_rows, :],
            dst_ref=kv_buf.at[g, :, my_rows, :],
            send_sem=kv_send.at[g, k],
            recv_sem=kv_recv.at[g, k],
            device_id={"ctx": peer},
            device_id_type=MESH,
        )

    def kv_arrival(g, k):
        peer = lax.rem(me + ctx_count - k, ctx_count)
        its_rows = pl.ds(pl.multiple_of(peer * rows, rows), rows)
        landed = kv_buf.at[g, :, its_rows, :]
        return pltpu.make_async_remote_copy(
            src_ref=landed, dst_ref=landed, send_sem=kv_send.at[g, k], recv_sem=kv_recv.at[g, k],
            device_id={"ctx": peer}, device_id_type=MESH,
        )

    def moved_copy(kind, up):
        return pltpu.make_async_remote_copy(
            src_ref=q_buf.at[:, moved_cols] if kind else own_kv,
            dst_ref=(moved_q if kind else moved_kv).at[up],
            send_sem=moved_send.at[up, kind],
            recv_sem=moved_recv.at[up, kind],
            device_id={"dp": above if up else below},
            device_id_type=MESH,
        )

    local[0].wait()
    local[1].wait()
    moved_copy(0, 1).start()
    moved_copy(0, 0).start()
    for g in range(moved):
        local[2 * g + 2].wait()
        local[2 * g + 3].wait()
        for k in range(1, ctx_count):
            kv_copy(g, k).start()
        if g == 0:
            q_copy.wait()
            moved_copy(1, 1).start()
            moved_copy(1, 0).start()

    for copy in scalars:
        copy.wait()

    def ends_of(sequence):
        ends = []
        total_length = 0
        for d in range(docs):
            total_length = total_length + lengths_ref[sequence, d]
            ends.append(total_length)
        return ends

    own_ends = ends_of(dp_index)

    def identity_of(place, first_slot, settled):
        early = place < span
        position = jnp.where(
            early, order_ref[first_slot] * span, order_ref[first_slot + 1] * span - span
        ) + place
        partners = dest_ref[0, first_slot], dest_ref[0, first_slot + 1]
        counted = jnp.where(early, partners[0] * docs, partners[1] * docs)
        if settled:
            ends = [jnp.where(early, *pair) for pair in zip(ends_of(partners[0]), ends_of(partners[1]))]
        else:
            ends = own_ends
        for end in ends:
            counted = counted + (position >= end).astype(jnp.int32)
        return position, counted

    query_place = lax.broadcasted_iota(jnp.int32, (rows, rows), 0)
    key_place = lax.broadcasted_iota(jnp.int32, (1, rows), 1)
    for settled, target in ((False, bias), (True, settled_bias)):
        query_position, query_document = identity_of(query_place, 2 * me, settled)
        for b in range(ctx_count):
            key_position, key_document = identity_of(key_place, 2 * b, settled)
            visible = (key_document == query_document) & (key_position <= query_position)
            target[:, b * rows:(b + 1) * rows] = jnp.where(visible, 0.0, MASK_FLOOR)

    row_source = jnp.where(
        lax.broadcasted_iota(jnp.int32, (rows, HEAD_SIZE), 0) < span,
        dest_ref[0, 2 * me], dest_ref[0, 2 * me + 1],
    )
    is_below = row_source == below
    is_above = row_source == above

    def settle_rows(kept, lower, upper):
        chosen = jnp.where(
            is_below, lower.astype(jnp.float32),
            jnp.where(is_above, upper.astype(jnp.float32), kept.astype(jnp.float32)),
        )
        return chosen.astype(jnp.bfloat16)

    def out_copy(chunk, up):
        return pltpu.make_async_remote_copy(
            src_ref=own.at[chunk],
            dst_ref=(from_below if up else from_above).at[chunk],
            send_sem=out_send.at[up, chunk],
            recv_sem=out_recv.at[up, chunk],
            device_id={"dp": above if up else below},
            device_id_type=MESH,
        )

    def send(chunk):
        out_copy(chunk, 1).start()
        out_copy(chunk, 0).start()

    exponent_scale = math.log2(math.e) / math.sqrt(HEAD_SIZE)

    def attend(query, g, mask):
        scores = lax.dot_general(
            query, kv_buf[g, 0], (((1,), (1,)), ((), ())), preferred_element_type=jnp.float32
        ) + mask[...]
        row_max = jnp.max(scores, axis=1, keepdims=True)
        weights = jnp.exp2((scores - row_max) * exponent_scale)
        total = jnp.sum(weights, axis=1, keepdims=True)
        mixed = jnp.dot(
            weights.astype(jnp.bfloat16), kv_buf[g, 1], preferred_element_type=jnp.float32
        )
        return (mixed / total).astype(jnp.bfloat16)

    for g in range(moved):
        for k in range(1, ctx_count):
            kv_arrival(g, k).wait_recv()

        def one_chunk(i, carry):
            chunk = g * group_chunks + i
            for j in range(CHUNK_HEADS):
                first = pl.multiple_of(chunk * chunk_cols + j * HEAD_SIZE, HEAD_SIZE)
                own[chunk, :, j * HEAD_SIZE:(j + 1) * HEAD_SIZE] = attend(
                    q_buf[:, pl.ds(first, HEAD_SIZE)], g, bias
                )
                if j == 0:
                    if g == 0:
                        @pl.when(i > 0)
                        def _():
                            send(chunk - 1)
                    else:
                        send(chunk - 1)
            return carry

        if g == moved - 1:
            for k in range(1, ctx_count):
                kv_copy(moved, k).start()
        lax.fori_loop(0, group_chunks, one_chunk, 0)
        if g == max(moved - 2, 0):
            moved_copy(0, 1).wait_recv()
            moved_copy(0, 0).wait_recv()
            for part in range(2):
                kv_buf[moved, part, my_rows, :] = settle_rows(
                    own_kv[part], moved_kv[1, part], moved_kv[0, part]
                )
    send(chunks - 1)

    moved_copy(1, 1).wait_recv()
    moved_copy(1, 0).wait_recv()
    for k in range(1, ctx_count):
        kv_arrival(moved, k).wait_recv()

    def one_moved(i, carry):
        for j in range(CHUNK_HEADS):
            inner = pl.ds(pl.multiple_of(i * chunk_cols + j * HEAD_SIZE, HEAD_SIZE), HEAD_SIZE)
            outer = pl.ds(
                pl.multiple_of(chunks * chunk_cols + i * chunk_cols + j * HEAD_SIZE, HEAD_SIZE),
                HEAD_SIZE,
            )
            query = settle_rows(q_buf[:, outer], moved_q[1, :, inner], moved_q[0, :, inner])
            out_ref[0, :, outer] = attend(query, moved, settled_bias)
        return carry

    lax.fori_loop(0, group_chunks, one_moved, 0)

    def settle(chunk, carry):
        out_copy(chunk, 1).wait_recv()
        out_copy(chunk, 0).wait_recv()
        for j in range(CHUNK_HEADS):
            first = pl.multiple_of(chunk * chunk_cols + j * HEAD_SIZE, HEAD_SIZE)
            part = pl.ds(j * HEAD_SIZE, HEAD_SIZE)
            out_ref[0, :, pl.ds(first, HEAD_SIZE)] = settle_rows(
                own[chunk, :, part], from_below[chunk, :, part], from_above[chunk, :, part]
            )
        return carry

    lax.fori_loop(0, chunks, settle, 0)

    for kind in range(2):
        for up in range(2):
            moved_copy(kind, up).wait_send()
    for g in range(KEY_VALUE_HEADS):
        for k in range(1, ctx_count):
            kv_copy(g, k).wait_send()

    def drain(chunk, carry):
        out_copy(chunk, 1).wait_send()
        out_copy(chunk, 0).wait_send()
        return carry

    lax.fori_loop(0, chunks, drain, 0)


def place_kernel(settled_ref, out_ref, sems):
    rows = settled_ref.shape[1] // PLACE_PARTS
    copies = [
        pltpu.make_async_copy(
            settled_ref.at[0, pl.ds(i * rows, rows), :],
            out_ref.at[0, pl.ds(i * rows, rows), :],
            sems.at[i],
        )
        for i in range(PLACE_PARTS)
    ]
    for copy in copies:
        copy.start()
    for copy in copies:
        copy.wait()


def on_device(dp_count, ctx_count, qkv, dest, order, lengths):
    rows = qkv.shape[1]
    query_width = QUERY_HEADS * HEAD_SIZE
    group_width = QUERIES_PER_KV * HEAD_SIZE
    chunks = (QUERY_HEADS - QUERIES_PER_KV) // CHUNK_HEADS
    chunk_shape = (chunks, rows, CHUNK_HEADS * HEAD_SIZE)
    keys = ctx_count * rows
    qkv, dest, order, lengths = (
        pltpu.with_memory_space_constraint(array, pltpu.HBM)
        for array in (qkv, dest, order, lengths)
    )
    settled = pl.pallas_call(
        functools.partial(kernel, dp_count, ctx_count),
        out_shape=pltpu.VMEM((1, rows, query_width), jnp.bfloat16),
        in_specs=[pl.BlockSpec(memory_space=pltpu.HBM)] * 4,
        out_specs=pl.BlockSpec(memory_space=pltpu.VMEM),
        scratch_shapes=[
            pltpu.SMEM(dest.shape, jnp.int32),
            pltpu.SMEM(order.shape, jnp.int32),
            pltpu.SMEM(lengths.shape, jnp.int32),
            pltpu.VMEM((rows, query_width), jnp.bfloat16),
            pltpu.VMEM((KEY_VALUE_HEADS, 2, keys, HEAD_SIZE), jnp.bfloat16),
            pltpu.VMEM((rows, keys), jnp.float32),
            pltpu.VMEM((rows, keys), jnp.float32),
            pltpu.VMEM(chunk_shape, jnp.bfloat16),
            pltpu.VMEM(chunk_shape, jnp.bfloat16),
            pltpu.VMEM(chunk_shape, jnp.bfloat16),
            pltpu.VMEM((2, rows, group_width), jnp.bfloat16),
            pltpu.VMEM((2, 2, rows, HEAD_SIZE), jnp.bfloat16),
            pltpu.VMEM((2, rows, HEAD_SIZE), jnp.bfloat16),
            pltpu.SemaphoreType.DMA((2 * KEY_VALUE_HEADS + 1,)),
            pltpu.SemaphoreType.DMA((3,)),
            pltpu.SemaphoreType.DMA((KEY_VALUE_HEADS, ctx_count)),
            pltpu.SemaphoreType.DMA((KEY_VALUE_HEADS, ctx_count)),
            pltpu.SemaphoreType.DMA((2, chunks)),
            pltpu.SemaphoreType.DMA((2, chunks)),
            pltpu.SemaphoreType.DMA((2, 2)),
            pltpu.SemaphoreType.DMA((2, 2)),
        ],
        compiler_params=pltpu.CompilerParams(collective_id=0, has_side_effects=True,
            vmem_limit_bytes=40 << 20),
    )(qkv, dest, order, lengths)
    return pl.pallas_call(
        place_kernel,
        out_shape=jax.ShapeDtypeStruct((1, rows, query_width), jnp.bfloat16),
        in_specs=[pl.BlockSpec(memory_space=pltpu.VMEM)],
        out_specs=pl.BlockSpec(memory_space=pltpu.HBM),
        scratch_shapes=[pltpu.SemaphoreType.DMA((PLACE_PARTS,))],
        compiler_params=pltpu.CompilerParams(vmem_limit_bytes=8 << 20),
    )(settled)


def solution(mesh):
    return jax.shard_map(
        functools.partial(on_device, mesh.shape["dp"], mesh.shape["ctx"]),
        mesh=mesh,
        in_specs=(P("dp", "ctx", None), P("dp", None), P(), P()),
        out_specs=P("dp", "ctx", None),
        check_vma=False,
    )
```

```python
import functools
import math

import jax
import jax.numpy as jnp
from jax import lax
from jax.experimental import pallas as pl
from jax.experimental.pallas import tpu as pltpu
from jax.sharding import PartitionSpec as P

QUERY_HEADS = 32
KEY_VALUE_HEADS = 4
HEAD_SIZE = 128
QUERIES_PER_KV = 8
CHUNK_HEADS = 4
PLACE_PARTS = 4

MASK_FLOOR = -1e30
MESH = pl.DeviceIdType.MESH


def kernel(
    dp_count, ctx_count,
    qkv_ref, dest_hbm, order_hbm, lengths_hbm,
    out_ref,
    dest_ref, order_ref, lengths_ref, q_buf, kv_buf, bias, settled_bias, own, from_below, from_above,
    moved_q, moved_kv, own_kv,
    local_sem, scalar_sem, kv_send, kv_recv, out_send, out_recv, moved_send, moved_recv, corner_sem,
):
    dp_index = lax.axis_index("dp")
    me = lax.axis_index("ctx")
    above = lax.rem(dp_index + 1, dp_count)
    below = lax.rem(dp_index + dp_count - 1, dp_count)
    rows = qkv_ref.shape[1]
    span = rows // 2
    docs = lengths_ref.shape[1]
    query_width = QUERY_HEADS * HEAD_SIZE
    chunk_cols = CHUNK_HEADS * HEAD_SIZE
    moved = KEY_VALUE_HEADS - 1
    group_chunks = QUERIES_PER_KV // CHUNK_HEADS
    chunks = moved * group_chunks
    moved_cols = pl.ds(moved * QUERIES_PER_KV * HEAD_SIZE, QUERIES_PER_KV * HEAD_SIZE)
    my_rows = pl.ds(pl.multiple_of(me * rows, rows), rows)

    square = ctx_count == 4
    corner = 3

    def target_of(k):
        if square:
            return (me + 1 - 2 * lax.rem(me, 2), lax.rem(me + 2, 4), 3 - me)[k - 1]
        return lax.rem(me + k, ctx_count)

    def origin_of(k):
        return target_of(k) if square else lax.rem(me + ctx_count - k, ctx_count)

    barrier = pltpu.get_barrier_semaphore()
    pl.semaphore_signal(barrier, inc=1, device_id={"dp": above}, device_id_type=MESH)
    pl.semaphore_signal(barrier, inc=1, device_id={"dp": below}, device_id_type=MESH)
    for k in range(1, corner if square else ctx_count):
        pl.semaphore_signal(barrier, inc=1, device_id={"ctx": target_of(k)}, device_id_type=MESH)
    scalars = [
        pltpu.make_async_copy(source, target, scalar_sem.at[i])
        for i, (source, target) in enumerate(
            ((dest_hbm, dest_ref), (order_hbm, order_ref), (lengths_hbm, lengths_ref))
        )
    ]
    local = []
    for g in (moved, *range(moved)):
        for part in range(2):
            first = query_width + (part * KEY_VALUE_HEADS + g) * HEAD_SIZE
            copy = pltpu.make_async_copy(
                qkv_ref.at[0, :, pl.ds(first, HEAD_SIZE)],
                own_kv.at[part] if g == moved else kv_buf.at[g, part, my_rows, :],
                local_sem.at[2 * g + part],
            )
            copy.start()
            local.append(copy)
        if g == moved:
            q_copy = pltpu.make_async_copy(
                qkv_ref.at[0, :, pl.ds(0, query_width)], q_buf, local_sem.at[2 * KEY_VALUE_HEADS]
            )
            q_copy.start()
    for copy in scalars:
        copy.start()

    pl.semaphore_wait(barrier, 4 if square else ctx_count + 1)
    if square:
        pl.semaphore_signal(corner_sem, inc=1, device_id={"ctx": target_of(1)}, device_id_type=MESH)

    def kv_copy(g, k):
        peer = target_of(k)
        return pltpu.make_async_remote_copy(
            src_ref=kv_buf.at[g, :, my_rows, :],
            dst_ref=kv_buf.at[g, :, my_rows, :],
            send_sem=kv_send.at[g, k],
            recv_sem=kv_recv.at[g, k],
            device_id={"ctx": peer},
            device_id_type=MESH,
        )

    def kv_arrival(g, k):
        peer = origin_of(k)
        its_rows = pl.ds(pl.multiple_of(peer * rows, rows), rows)
        landed = kv_buf.at[g, :, its_rows, :]
        return pltpu.make_async_remote_copy(
            src_ref=landed, dst_ref=landed, send_sem=kv_send.at[g, k], recv_sem=kv_recv.at[g, k],
            device_id={"ctx": peer}, device_id_type=MESH,
        )

    def moved_copy(kind, up):
        return pltpu.make_async_remote_copy(
            src_ref=q_buf.at[:, moved_cols] if kind else own_kv,
            dst_ref=(moved_q if kind else moved_kv).at[up],
            send_sem=moved_send.at[up, kind],
            recv_sem=moved_recv.at[up, kind],
            device_id={"dp": above if up else below},
            device_id_type=MESH,
        )

    local[0].wait()
    local[1].wait()
    moved_copy(0, 1).start()
    moved_copy(0, 0).start()
    for g in range(moved):
        local[2 * g + 2].wait()
        local[2 * g + 3].wait()
        for k in range(1, ctx_count):
            if g == 0 and k == ctx_count - 1:
                q_copy.wait()
                moved_copy(1, 1).start()
                moved_copy(1, 0).start()
                if square:
                    pl.semaphore_wait(corner_sem, 1)
            kv_copy(g, k).start()

    for copy in scalars:
        copy.wait()

    def ends_of(sequence):
        ends = []
        total_length = 0
        for d in range(docs):
            total_length = total_length + lengths_ref[sequence, d]
            ends.append(total_length)
        return ends

    own_ends = ends_of(dp_index)

    def identity_of(place, first_slot, settled):
        early = place < span
        position = jnp.where(
            early, order_ref[first_slot] * span, order_ref[first_slot + 1] * span - span
        ) + place
        partners = dest_ref[0, first_slot], dest_ref[0, first_slot + 1]
        counted = jnp.where(early, partners[0] * docs, partners[1] * docs)
        if settled:
            ends = [jnp.where(early, *pair) for pair in zip(ends_of(partners[0]), ends_of(partners[1]))]
        else:
            ends = own_ends
        for end in ends:
            counted = counted + (position >= end).astype(jnp.int32)
        return position, counted

    query_place = lax.broadcasted_iota(jnp.int32, (rows, rows), 0)
    key_place = lax.broadcasted_iota(jnp.int32, (1, rows), 1)
    for settled, target in ((False, bias), (True, settled_bias)):
        query_position, query_document = identity_of(query_place, 2 * me, settled)
        for b in range(ctx_count):
            key_position, key_document = identity_of(key_place, 2 * b, settled)
            visible = (key_document == query_document) & (key_position <= query_position)
            target[:, b * rows:(b + 1) * rows] = jnp.where(visible, 0.0, MASK_FLOOR)

    row_source = jnp.where(
        lax.broadcasted_iota(jnp.int32, (rows, HEAD_SIZE), 0) < span,
        dest_ref[0, 2 * me], dest_ref[0, 2 * me + 1],
    )
    is_below = row_source == below
    is_above = row_source == above

    def settle_rows(kept, lower, upper):
        chosen = jnp.where(
            is_below, lower.astype(jnp.float32),
            jnp.where(is_above, upper.astype(jnp.float32), kept.astype(jnp.float32)),
        )
        return chosen.astype(jnp.bfloat16)

    def out_copy(chunk, up):
        return pltpu.make_async_remote_copy(
            src_ref=own.at[chunk],
            dst_ref=(from_below if up else from_above).at[chunk],
            send_sem=out_send.at[up, chunk],
            recv_sem=out_recv.at[up, chunk],
            device_id={"dp": above if up else below},
            device_id_type=MESH,
        )

    def send(chunk):
        out_copy(chunk, 1).start()
        out_copy(chunk, 0).start()

    exponent_scale = math.log2(math.e) / math.sqrt(HEAD_SIZE)

    def attend(query, g, mask):
        scores = lax.dot_general(
            query, kv_buf[g, 0], (((1,), (1,)), ((), ())), preferred_element_type=jnp.float32
        ) + mask[...]
        row_max = jnp.max(scores, axis=1, keepdims=True)
        weights = jnp.exp2((scores - row_max) * exponent_scale)
        total = jnp.sum(weights, axis=1, keepdims=True)
        mixed = jnp.dot(
            weights.astype(jnp.bfloat16), kv_buf[g, 1], preferred_element_type=jnp.float32
        )
        return (mixed / total).astype(jnp.bfloat16)

    for g in range(moved):
        for k in range(1, ctx_count):
            kv_arrival(g, k).wait_recv()

        def one_chunk(i, carry):
            chunk = g * group_chunks + i
            for j in range(CHUNK_HEADS):
                first = pl.multiple_of(chunk * chunk_cols + j * HEAD_SIZE, HEAD_SIZE)
                own[chunk, :, j * HEAD_SIZE:(j + 1) * HEAD_SIZE] = attend(
                    q_buf[:, pl.ds(first, HEAD_SIZE)], g, bias
                )
                if j == 0:
                    if g == 0:
                        @pl.when(i > 0)
                        def _():
                            send(chunk - 1)
                    else:
                        send(chunk - 1)
            return carry

        if g == moved - 1:
            for k in range(1, ctx_count):
                kv_copy(moved, k).start()
        lax.fori_loop(0, group_chunks, one_chunk, 0)
        if g == max(moved - 2, 0):
            moved_copy(0, 1).wait_recv()
            moved_copy(0, 0).wait_recv()
            for part in range(2):
                kv_buf[moved, part, my_rows, :] = settle_rows(
                    own_kv[part], moved_kv[1, part], moved_kv[0, part]
                )
    send(chunks - 1)

    moved_copy(1, 1).wait_recv()
    moved_copy(1, 0).wait_recv()
    for k in range(1, ctx_count):
        kv_arrival(moved, k).wait_recv()

    def one_moved(i, carry):
        for j in range(CHUNK_HEADS):
            inner = pl.ds(pl.multiple_of(i * chunk_cols + j * HEAD_SIZE, HEAD_SIZE), HEAD_SIZE)
            outer = pl.ds(
                pl.multiple_of(chunks * chunk_cols + i * chunk_cols + j * HEAD_SIZE, HEAD_SIZE),
                HEAD_SIZE,
            )
            query = settle_rows(q_buf[:, outer], moved_q[1, :, inner], moved_q[0, :, inner])
            out_ref[0, :, outer] = attend(query, moved, settled_bias)
        return carry

    lax.fori_loop(0, group_chunks, one_moved, 0)

    def settle(chunk, carry):
        out_copy(chunk, 1).wait_recv()
        out_copy(chunk, 0).wait_recv()
        for j in range(CHUNK_HEADS):
            first = pl.multiple_of(chunk * chunk_cols + j * HEAD_SIZE, HEAD_SIZE)
            part = pl.ds(j * HEAD_SIZE, HEAD_SIZE)
            out_ref[0, :, pl.ds(first, HEAD_SIZE)] = settle_rows(
                own[chunk, :, part], from_below[chunk, :, part], from_above[chunk, :, part]
            )
        return carry

    lax.fori_loop(0, chunks, settle, 0)

    for kind in range(2):
        for up in range(2):
            moved_copy(kind, up).wait_send()
    for g in range(KEY_VALUE_HEADS):
        for k in range(1, ctx_count):
            kv_copy(g, k).wait_send()

    def drain(chunk, carry):
        out_copy(chunk, 1).wait_send()
        out_copy(chunk, 0).wait_send()
        return carry

    lax.fori_loop(0, chunks, drain, 0)


def place_kernel(settled_ref, out_ref, sems):
    rows = settled_ref.shape[1] // PLACE_PARTS
    copies = [
        pltpu.make_async_copy(
            settled_ref.at[0, pl.ds(i * rows, rows), :],
            out_ref.at[0, pl.ds(i * rows, rows), :],
            sems.at[i],
        )
        for i in range(PLACE_PARTS)
    ]
    for copy in copies:
        copy.start()
    for copy in copies:
        copy.wait()


def on_device(dp_count, ctx_count, qkv, dest, order, lengths):
    rows = qkv.shape[1]
    query_width = QUERY_HEADS * HEAD_SIZE
    group_width = QUERIES_PER_KV * HEAD_SIZE
    chunks = (QUERY_HEADS - QUERIES_PER_KV) // CHUNK_HEADS
    chunk_shape = (chunks, rows, CHUNK_HEADS * HEAD_SIZE)
    keys = ctx_count * rows
    qkv, dest, order, lengths = (
        pltpu.with_memory_space_constraint(array, pltpu.HBM)
        for array in (qkv, dest, order, lengths)
    )
    settled = pl.pallas_call(
        functools.partial(kernel, dp_count, ctx_count),
        out_shape=pltpu.VMEM((1, rows, query_width), jnp.bfloat16),
        in_specs=[pl.BlockSpec(memory_space=pltpu.HBM)] * 4,
        out_specs=pl.BlockSpec(memory_space=pltpu.VMEM),
        scratch_shapes=[
            pltpu.SMEM(dest.shape, jnp.int32),
            pltpu.SMEM(order.shape, jnp.int32),
            pltpu.SMEM(lengths.shape, jnp.int32),
            pltpu.VMEM((rows, query_width), jnp.bfloat16),
            pltpu.VMEM((KEY_VALUE_HEADS, 2, keys, HEAD_SIZE), jnp.bfloat16),
            pltpu.VMEM((rows, keys), jnp.float32),
            pltpu.VMEM((rows, keys), jnp.float32),
            pltpu.VMEM(chunk_shape, jnp.bfloat16),
            pltpu.VMEM(chunk_shape, jnp.bfloat16),
            pltpu.VMEM(chunk_shape, jnp.bfloat16),
            pltpu.VMEM((2, rows, group_width), jnp.bfloat16),
            pltpu.VMEM((2, 2, rows, HEAD_SIZE), jnp.bfloat16),
            pltpu.VMEM((2, rows, HEAD_SIZE), jnp.bfloat16),
            pltpu.SemaphoreType.DMA((2 * KEY_VALUE_HEADS + 1,)),
            pltpu.SemaphoreType.DMA((3,)),
            pltpu.SemaphoreType.DMA((KEY_VALUE_HEADS, ctx_count)),
            pltpu.SemaphoreType.DMA((KEY_VALUE_HEADS, ctx_count)),
            pltpu.SemaphoreType.DMA((2, chunks)),
            pltpu.SemaphoreType.DMA((2, chunks)),
            pltpu.SemaphoreType.DMA((2, 2)),
            pltpu.SemaphoreType.DMA((2, 2)),
            pltpu.SemaphoreType.REGULAR,
        ],
        compiler_params=pltpu.CompilerParams(collective_id=0, has_side_effects=True,
            vmem_limit_bytes=40 << 20),
    )(qkv, dest, order, lengths)
    return pl.pallas_call(
        place_kernel,
        out_shape=jax.ShapeDtypeStruct((1, rows, query_width), jnp.bfloat16),
        in_specs=[pl.BlockSpec(memory_space=pltpu.VMEM)],
        out_specs=pl.BlockSpec(memory_space=pltpu.HBM),
        scratch_shapes=[pltpu.SemaphoreType.DMA((PLACE_PARTS,))],
        compiler_params=pltpu.CompilerParams(vmem_limit_bytes=8 << 20),
    )(settled)


def solution(mesh):
    return jax.shard_map(
        functools.partial(on_device, mesh.shape["dp"], mesh.shape["ctx"]),
        mesh=mesh,
        in_specs=(P("dp", "ctx", None), P("dp", None), P(), P()),
        out_specs=P("dp", "ctx", None),
        check_vma=False,
    )
```
